32 devices in a mesh: seq: 8 (over z, y), head: 4 (over x, core).
Axes of the slice: x: 2, y: 2, z: 4, core: 2. Of those that a mesh axis runs over, the one named last changes fastest.
Arguments:
- q_low: bfloat16 [2048, 1536], P('seq', 'head'), may hold values from -500 to 500
- q_gain: bfloat16 [1536], P('head'), may hold values from 0.099609375 to 1.8984375
- q_up: bfloat16 [1536, 24576], P(None, 'head'), may hold values from -0.15625 to 0.15625
- key_absorb: bfloat16 [128, 128, 512], P('head'), may hold values from -0.5 to 0.5
- value_absorb: bfloat16 [128, 512, 128], P('head'), may hold values from -0.25 to 0.25
- latent_cache: bfloat16 [65536, 576], P('seq'), may hold values from -1300 to 1300
- tile_picks: int32 [16, 16], P('seq'), may hold values from 0 to 511, as said below
Outputs:
- attended: bfloat16 [2048, 16384], P('seq', 'head')
The draws below stay inside these ranges and needn't reach their ends.
Inputs may be any that keep to these rules, and one draw needn't show every extreme that they name: `tile_picks`: the 16 tiles of one query block differ. Of all tiles that the query blocks of one index of seq select together, at most 8 lie in the cache rows of one index of seq, and exactly 8 in those of some index.
All inputs are finite; a program needn't handle non-finite values.
Results may differ from the reference program's by a relative error of at most 0.03.
Values may be sent and summed in bfloat16 or wider, within the bound.
A program may use at most 192 MiB of HBM per device.

```python
import math
import jax
import jax.numpy as jnp
from jax import lax

HEADS = 128
NOPE = 128
ROPE = 64
LATENT = 512
VDIM = 128
QLORA = 1536
TILE = 128
TOPT = 16
QBLK = 128
CACHE_DEV = 8192
Q_DEV = 256
TOKENS = 2048
CONTEXT = 65536
CAP = 8


def draw_q_low(key, part):
    keys = jax.random.split(key, 3)
    row_scale = jnp.exp(jax.random.uniform(keys[0], (TOKENS, 1), jnp.float32, 0.0, math.log(10.0)))
    column_scale = jnp.exp(jax.random.uniform(keys[1], (1, QLORA), jnp.float32, 0.0, math.log(10.0)))
    base = jnp.clip(jax.random.normal(keys[2], (TOKENS, QLORA), jnp.float32), -5.0, 5.0)
    return (base * row_scale * column_scale).astype(jnp.bfloat16)


def draw_latent_cache(key, part):
    keys = jax.random.split(key, 1)
    width = LATENT + ROPE
    base = jnp.clip(jax.random.normal(keys[0], (CONTEXT, width), jnp.float32), -6.0, 6.0)
    return base.astype(jnp.bfloat16)


def draw_tile_picks(key, part):
    devices = TOKENS // Q_DEV
    count = Q_DEV // QBLK * TOPT
    tiles_dev = CACHE_DEV // TILE
    stride = tiles_dev // CAP

    def one_device(device_key):
        keys = jax.random.split(device_key, 5)
        favoured = jax.random.randint(keys[0], (), 0, devices)
        order = jax.random.permutation(keys[1], devices * CAP)
        ranked = jnp.where(order // CAP == favoured, 0, 1).astype(jnp.int32)
        chosen = order[jnp.argsort(ranked, stable=True)][:count]
        owner = chosen // CAP
        occurrence = chosen % CAP
        offset = jax.random.randint(keys[2], (devices,), 0, tiles_dev)
        inside = jax.random.randint(keys[3], (count,), 0, stride)
        local = (offset[owner] + occurrence * stride + inside) % tiles_dev
        tiles = owner * tiles_dev + local
        tiles = tiles[jax.random.permutation(keys[4], count)]
        return tiles.reshape(Q_DEV // QBLK, TOPT).astype(jnp.int32)
    return jax.vmap(one_device)(jax.random.split(key, devices)).reshape(TOKENS // QBLK, TOPT)


def block_levels(rng, extent, shards, smallest, largest):
    loudness = 1.0
    for axis_at, parts in shards:
        draws = jax.random.uniform(jax.random.fold_in(jax.random.fold_in(rng, 6), axis_at), (parts,), jnp.float32, smallest / len(shards), largest / len(shards))
        loudness = loudness * jnp.repeat(jnp.exp(draws), extent[axis_at] // parts).reshape((-1,) + (1,) * (len(extent) - 1 - axis_at))
    return loudness


def bell_draw(own_key, dims, deviation, limit, cuts=(), kind=jnp.bfloat16):
    drawn = deviation * jax.random.normal(own_key, dims, jnp.float32)
    if cuts:
        drawn = drawn * block_levels(own_key, dims, cuts, -0.22, 0.18)
    return jnp.clip(drawn, -limit, limit).astype(kind)


def setup_inputs(seed: int = 0) -> dict:
    splits = jax.random.split(jax.random.key(seed), 8)
    return {
        "q_low": draw_q_low(jax.random.fold_in(splits[7], 71), 0),
        "q_gain": jnp.clip(1.0 + 0.18 * jax.random.normal(splits[1], (QLORA,), jnp.float32), 0.099609375, 1.8984375).astype(jnp.bfloat16),
        "q_up": bell_draw(splits[2], (QLORA, HEADS * (NOPE + ROPE)), QLORA ** -0.5, 0.15625, ((1, 4),)),
        "key_absorb": bell_draw(splits[3], (HEADS, NOPE, LATENT), NOPE ** -0.5, 0.5, ((0, 4),)),
        "value_absorb": bell_draw(splits[4], (HEADS, LATENT, VDIM), LATENT ** -0.5, 0.25, ((0, 4),)),
        "latent_cache": draw_latent_cache(jax.random.fold_in(splits[7], 71), 0),
        "tile_picks": draw_tile_picks(jax.random.fold_in(splits[7], 71), 0),
    }


def rms_normed(q_low, q_gain):
    values = q_low.astype(jnp.float32)
    power = lax.optimization_barrier(jnp.mean(values * values, axis=-1, keepdims=True))
    return (values * lax.rsqrt(power + 1e-06) * q_gain.astype(jnp.float32)).astype(jnp.bfloat16)

def rotate(rope, positions):
    half = rope.shape[-1] // 2
    freq = jnp.power(jnp.float32(10000.0), -(2.0 * jnp.arange(half, dtype=jnp.float32)) / rope.shape[-1])
    angle = positions.astype(jnp.float32)[:, None] * freq[None, :]
    cosine = jnp.cos(angle)[:, None, :]
    sine = jnp.sin(angle)[:, None, :]
    first = rope[..., :half].astype(jnp.float32)
    second = rope[..., half:].astype(jnp.float32)
    return jnp.concatenate([first * cosine - second * sine, first * sine + second * cosine], axis=-1).astype(jnp.bfloat16)

def reference(q_low, q_gain, q_up, key_absorb, value_absorb, latent_cache, tile_picks):
    tokens = q_low.shape[0]
    width = latent_cache.shape[1]
    normed = rms_normed(q_low, q_gain)
    query = jnp.dot(normed, q_up, preferred_element_type=jnp.float32).astype(jnp.bfloat16)
    query = query.reshape(tokens, HEADS, NOPE + ROPE)
    positions = CONTEXT + jnp.arange(tokens, dtype=jnp.int32)
    rotated = rotate(query[..., NOPE:], positions)
    latent_q = jnp.einsum('thn,hnl->thl', query[..., :NOPE].astype(jnp.float32), key_absorb.astype(jnp.float32)).astype(jnp.bfloat16)
    full_q = jnp.concatenate([latent_q, rotated], axis=-1).reshape(tokens // QBLK, QBLK * HEADS, width)
    tiles = latent_cache.reshape(CONTEXT // TILE, TILE, width)
    scale = float(NOPE + ROPE) ** (-0.5)

    def one_block(operands):
        block_q, picks = operands
        keys = jnp.take(tiles, picks.astype(jnp.int32), axis=0).reshape(TOPT * TILE, width)
        scores = jnp.dot(block_q, keys.T, preferred_element_type=jnp.float32) * scale
        weights = jax.nn.softmax(scores, axis=-1).astype(jnp.bfloat16)
        return jnp.dot(weights, keys[:, :LATENT], preferred_element_type=jnp.float32).astype(jnp.bfloat16)
    mixed = lax.map(one_block, (full_q, tile_picks)).reshape(tokens, HEADS, LATENT)
    attended = jnp.einsum('thl,hlv->thv', mixed.astype(jnp.float32), value_absorb.astype(jnp.float32))
    return attended.astype(jnp.bfloat16).reshape(tokens, HEADS * VDIM)
```

```python
import functools

import jax
import jax.numpy as jnp
from jax import lax
from jax.experimental import pallas as pl
from jax.experimental.pallas import tpu as pltpu
from jax.sharding import PartitionSpec as P

NOPE = 128
ROPE = 64
LATENT = 512
VDIM = 128
TILE = 128
TOPT = 16
QBLK = 128
LANES = 128
SUBLANES = 16
LOG2E = 1.4426950408889634
MESH = pl.DeviceIdType.MESH


def rotary_tables(positions):
    half = ROPE // 2
    freq = jnp.power(
        jnp.float32(10000.0), -(2.0 * jnp.arange(half, dtype=jnp.float32)) / ROPE
    )
    angle = positions.astype(jnp.float32)[:, None] * freq[None, :]
    cosine, sine = jnp.cos(angle), jnp.sin(angle)
    return (
        jnp.concatenate([cosine, cosine], axis=-1),
        jnp.concatenate([-sine, sine], axis=-1),
    )


def request_kernel(n, ask_ref, serve_ref, send, recv):
    me = lax.axis_index("seq")
    barrier = pltpu.get_barrier_semaphore()
    for shift in range(1, n):
        pl.semaphore_signal(
            barrier, inc=1, device_id={"seq": lax.rem(me + shift, n)}, device_id_type=MESH
        )
    pl.semaphore_wait(barrier, n - 1)
    copies = []
    for shift in range(1, n):
        peer = lax.rem(me + shift, n)
        copies.append(
            pltpu.make_async_remote_copy(
                src_ref=ask_ref.at[peer],
                dst_ref=serve_ref.at[me],
                send_sem=send.at[shift],
                recv_sem=recv.at[shift],
                device_id={"seq": peer},
                device_id_type=MESH,
            )
        )
        copies[-1].start()
    serve_ref[me] = ask_ref[me]
    for copy in copies:
        copy.wait()


def exchange_requests(ask):
    n = ask.shape[0]
    return pl.pallas_call(
        functools.partial(request_kernel, n),
        out_shape=jax.ShapeDtypeStruct(ask.shape, ask.dtype),
        in_specs=[pl.BlockSpec(memory_space=pltpu.VMEM)],
        out_specs=pl.BlockSpec(memory_space=pltpu.VMEM),
        scratch_shapes=[pltpu.SemaphoreType.DMA((n,)), pltpu.SemaphoreType.DMA((n,))],
        compiler_params=pltpu.CompilerParams(collective_id=0, has_side_effects=True),
        name="requests",
    )(ask)


def main_kernel(
    dims,
    early_ref,
    late_ref,
    found_ref,
    low_ref,
    up_hbm,
    key_hbm,
    value_hbm,
    cos_ref,
    sin_ref,
    out_ref,
    land_a,
    land_b,
    lows,
    normed,
    up_buf,
    key_buf,
    value_buf,
    full_q,
    turned,
    values,
    part,
    part_top,
    part_sum,
    send_a,
    recv_a,
    send_x,
    recv_x,
    send_p,
    recv_p,
    low_send,
    low_recv,
    weight_sem,
    up_sem,
):
    n, lanes_x, half, grain, rows, heads = dims
    subs = half // grain
    me = lax.axis_index("seq")
    place = lax.axis_index("head")
    column, core = place // 2, lax.rem(place, 2)
    mate = column * 2 + (1 - core)
    lands = (land_a, land_b)
    blocks = rows // QBLK

    def beside(step):
        return lax.rem(column + step, lanes_x) * 2 + core

    def behind(step):
        return lax.rem(column + lanes_x - step, lanes_x) * 2 + core

    barrier = pltpu.get_barrier_semaphore()
    for shift in range(1, n):
        pl.semaphore_signal(
            barrier, inc=1, device_id={"seq": lax.rem(me + shift, n)}, device_id_type=MESH
        )
    for step in range(1, lanes_x):
        pl.semaphore_signal(barrier, inc=1, device_id={"head": beside(step)}, device_id_type=MESH)
    pl.semaphore_signal(barrier, inc=1, device_id={"head": mate}, device_id_type=MESH)
    pl.semaphore_wait(barrier, n - 1 + lanes_x)

    def low_copy(src, slot, step, peer, index):
        return pltpu.make_async_remote_copy(
            src_ref=src,
            dst_ref=lows.at[slot],
            send_sem=low_send.at[index, step],
            recv_sem=low_recv.at[index, step],
            device_id={"head": peer},
            device_id_type=MESH,
        )

    low_own = pltpu.make_async_copy(low_ref, lows.at[place], low_recv.at[0, 0])
    low_own.start()
    for step in range(1, lanes_x):
        low_copy(low_ref, place, step, beside(step), 0).start()
    low_copy(low_ref, place, 0, mate, 1).start()

    def seq_copy(part_at, sub, shift):
        peer = lax.rem(me + shift, n)
        return pltpu.make_async_remote_copy(
            src_ref=found_ref.at[peer, pl.ds(part_at * half + sub * grain, grain)],
            dst_ref=lands[part_at].at[pl.ds(me * half + sub * grain, grain), place],
            send_sem=send_a.at[part_at, sub, shift],
            recv_sem=recv_a.at[part_at, sub, shift],
            device_id={"seq": peer},
            device_id_type=MESH,
        )

    def share(part_at, sub, shift, column_at):
        source = lax.rem(me + n - shift, n)
        return lands[part_at].at[pl.ds(source * half + sub * grain, grain), column_at]

    def side_copy(part_at, sub, shift, step):
        ref = share(part_at, sub, shift, place)
        return pltpu.make_async_remote_copy(
            src_ref=ref,
            dst_ref=ref,
            send_sem=send_x.at[part_at, sub, shift, step],
            recv_sem=recv_x.at[part_at, sub, shift, step],
            device_id={"head": beside(step)},
            device_id_type=MESH,
        )

    def mate_copy(part_at, sub, shift, step):
        ref = share(part_at, sub, shift, behind(step))
        return pltpu.make_async_remote_copy(
            src_ref=ref,
            dst_ref=ref,
            send_sem=send_p.at[part_at, sub, shift, step],
            recv_sem=recv_p.at[part_at, sub, shift, step],
            device_id={"head": mate},
            device_id_type=MESH,
        )

    def self_copy(part_at, sub):
        return pltpu.make_async_copy(
            found_ref.at[me, pl.ds(part_at * half + sub * grain, grain)],
            share(part_at, sub, 0, place),
            recv_a.at[part_at, sub, 0],
        )

    for part_at in range(2):
        for sub in range(subs):
            self_copy(part_at, sub).start()
            for shift in range(1, n):
                seq_copy(part_at, sub, shift).start()

    key_copy = pltpu.make_async_copy(key_hbm, key_buf, weight_sem.at[0])
    value_copy = pltpu.make_async_copy(value_hbm, value_buf, weight_sem.at[1])
    key_copy.start()
    value_copy.start()

    pair_width = 2 * (NOPE + ROPE)
    pairs = heads // 2

    def up_copy(index, slot):
        return pltpu.make_async_copy(
            up_hbm.at[:, pl.ds(pl.multiple_of(index * pair_width, LANES), pair_width)],
            up_buf.at[slot],
            up_sem.at[slot],
        )

    up_copy(0, 0).start()

    def pass_on(part_at, sub, shift):
        for step in range(1, lanes_x):
            side_copy(part_at, sub, shift, step).start()
        mate_copy(part_at, sub, shift, 0).start()

    def relay(part_at, sub, shift):
        for step in range(1, lanes_x):
            side_copy(part_at, sub, shift, step).wait_recv()
            mate_copy(part_at, sub, shift, step).start()

    items = subs * (n - 1)
    lag = 3

    def serve(part_at, item):
        sub, shift = item // (n - 1), 1 + lax.rem(item, n - 1)
        seq_copy(part_at, sub, shift).wait_recv()
        pass_on(part_at, sub, shift)

    def serve_relay(part_at, item):
        relay(part_at, item // (n - 1), 1 + lax.rem(item, n - 1))

    def advance(part_at, item):
        @pl.when(item < items)
        def _():
            serve(part_at, item)

        @pl.when((item >= lag) & (item < items + lag))
        def _():
            serve_relay(part_at, item - lag)

    for part_at in range(2):
        for sub in range(subs):
            self_copy(part_at, sub).wait()
            pass_on(part_at, sub, 0)

    low_own.wait()
    for step in range(1, lanes_x):
        low_copy(low_ref, place, step, beside(step), 0).wait_recv()
        slot = behind(step)
        low_copy(lows.at[slot], slot, step, mate, 1).start()
    for part_at in range(2):
        for sub in range(subs):
            relay(part_at, sub, 0)
    for step in range(lanes_x):
        low_copy(low_ref, place, step, mate, 1).wait_recv()

    shares = 2 * lanes_x
    wide = low_ref.shape[1]
    strip = 64

    @pl.loop(0, rows // strip)
    def _(index):
        span = pl.ds(pl.multiple_of(index * strip, strip), strip)
        pieces = [lows[slot, span, :].astype(jnp.float32) for slot in range(shares)]
        power = sum(jnp.sum(piece * piece, axis=-1, keepdims=True) for piece in pieces)
        inverse = lax.rsqrt(power / (wide * shares) + 1e-06)
        scaled = [
            piece * inverse * lows[slot, rows : rows + SUBLANES, :][:1].astype(jnp.float32)
            for slot, piece in enumerate(pieces)
        ]
        normed[span, :] = jnp.concatenate(scaled, axis=-1).astype(jnp.bfloat16)

    key_copy.wait()
    rope_half = ROPE // 2

    @pl.loop(0, pairs)
    def _(index):
        slot = lax.rem(index, 2)

        @pl.when(index + 1 < pairs)
        def _():
            up_copy(index + 1, lax.rem(index + 1, 2)).start()

        up_copy(index, slot).wait()
        query = jnp.dot(normed[...], up_buf[slot], preferred_element_type=jnp.float32).astype(
            jnp.bfloat16
        )
        cosine, sine = cos_ref[...], sin_ref[...]
        for head in range(2):
            start = head * (NOPE + ROPE)
            nope = query[:, start : start + NOPE]
            rope = query[:, start + NOPE : start + NOPE + ROPE].astype(jnp.float32)
            swapped = jnp.concatenate([rope[:, rope_half:], rope[:, :rope_half]], axis=-1)
            rotated = rope * cosine + swapped * sine
            full_q[index * 2 + head, :, :LATENT] = jnp.dot(
                nope, key_buf[index * 2 + head], preferred_element_type=jnp.float32
            ).astype(jnp.bfloat16)
            full_q[index * 2 + head, :, LATENT:] = jnp.concatenate(
                [rotated, jnp.zeros((rows, LANES - ROPE), jnp.float32)], axis=-1
            ).astype(jnp.bfloat16)

        @pl.when(lax.rem(index, 2) == 1)
        def _():
            advance(0, index // 2)

    width = LATENT + ROPE
    turned[width:, :] = jnp.zeros((turned.shape[0] - width, turned.shape[1]), turned.dtype)

    @pl.loop(pairs // 2, items + lag)
    def _(item):
        advance(0, item)

    def wait_mate(part_at):
        for sub in range(subs):
            @pl.loop(0, n)
            def _(shift):
                for step in range(lanes_x):
                    mate_copy(part_at, sub, shift, step).wait_recv()

    wait_mate(0)
    value_copy.wait()

    scale = float(NOPE + ROPE) ** (-0.5) * LOG2E
    step_heads = 4
    groups = heads // step_heads
    per = -(-(items + lag) // (2 * groups))
    count = TOPT // 2

    def place_tile(at, tile):
        tile = tile.reshape(width, TILE)
        turned[:width, at * TILE : (at + 1) * TILE] = tile
        values[at * TILE : (at + 1) * TILE, :] = tile[:LATENT].T

    def fill_early(block):
        for at in range(count):
            place_tile(at, land_a[early_ref[block * count + at]])

    def fill_late(block):
        for at in range(count):
            base = 3 * (block * count + at)
            first = land_a[late_ref[base]]
            second = land_b[late_ref[base + 1]]
            flag = jnp.full(first.shape, late_ref[base + 2], jnp.int32) > 0
            place_tile(at, jnp.where(flag, first, second))

    def attend(block, group, last):
        span = slice(block * QBLK, (block + 1) * QBLK)
        scores = []
        for at in range(0, step_heads, 2):
            queries = full_q[pl.ds(group * step_heads + at, 2), span].reshape(
                2 * QBLK, full_q.shape[2]
            )
            scores.append(jnp.dot(queries, turned[...], preferred_element_type=jnp.float32))
        for at in range(0, step_heads, 2):
            score = scores[at // 2]
            top = jnp.max(score, axis=-1, keepdims=True)
            weights = jnp.exp2((score - top) * scale)
            total = jnp.sum(weights, axis=-1, keepdims=True)
            mixed = jnp.dot(
                weights.astype(jnp.bfloat16), values[...], preferred_element_type=jnp.float32
            )
            mixed = (mixed / total).astype(jnp.bfloat16)
            for sub_head in range(2):
                head = group * step_heads + at + sub_head
                lines = slice(sub_head * QBLK, (sub_head + 1) * QBLK)
                result = jnp.dot(
                    mixed[lines], value_buf[head], preferred_element_type=jnp.float32
                )
                if not last:
                    part[block, head] = result
                    part_top[block, head] = top[lines]
                    part_sum[block, head] = total[lines]
                else:
                    old_top, old_sum = part_top[block, head], part_sum[block, head]
                    peak = jnp.maximum(old_top, top[lines])
                    old = old_sum * jnp.exp2((old_top - peak) * scale)
                    new = total[lines] * jnp.exp2((top[lines] - peak) * scale)
                    merged = (part[block, head] * old + result * new) / (old + new)
                    out_ref[
                        span, pl.ds(pl.multiple_of(head * VDIM, VDIM), VDIM)
                    ] = merged.astype(jnp.bfloat16)

    for block in range(blocks):
        fill_early(block)

        @pl.loop(0, groups)
        def _(group):
            attend(block, group, False)
            for extra in range(per):
                advance(1, (block * groups + group) * per + extra)

    wait_mate(1)
    for block in range(blocks):
        fill_late(block)

        @pl.loop(0, groups)
        def _(group):
            attend(block, group, True)

    for part_at in range(2):
        for sub in range(subs):
            @pl.loop(1, n)
            def _(shift):
                seq_copy(part_at, sub, shift).wait_send()

            @pl.loop(0, n)
            def _(shift):
                for step in range(1, lanes_x):
                    side_copy(part_at, sub, shift, step).wait_send()
                for step in range(lanes_x):
                    mate_copy(part_at, sub, shift, step).wait_send()
    for step in range(1, lanes_x):
        low_copy(low_ref, place, step, beside(step), 0).wait_send()
    for step in range(lanes_x):
        low_copy(low_ref, place, step, mate, 1).wait_send()


def exchange_and_attend(early, late, found, low, q_up, key_absorb, value_absorb, cosine, sine):
    n, cap, part_width, tile = found.shape
    head_count = lax.axis_size("head")
    half = cap // 2
    grain = max(1, half // 2)
    subs = half // grain
    lanes_x = head_count // 2
    heads = key_absorb.shape[0]
    rows = low.shape[0] - SUBLANES
    blocks = rows // QBLK
    depth = q_up.shape[0]
    padded = LATENT + LANES
    count = TOPT // 2 * TILE
    any_spec = pl.BlockSpec(memory_space=pl.ANY)
    vmem_spec = pl.BlockSpec(memory_space=pltpu.VMEM)
    smem_spec = pl.BlockSpec(memory_space=pltpu.SMEM)
    dma = pltpu.SemaphoreType.DMA
    land = pltpu.VMEM((n * half, head_count, part_width, tile), jnp.bfloat16)
    dims = (n, lanes_x, half, grain, rows, heads)
    return pl.pallas_call(
        functools.partial(main_kernel, dims),
        out_shape=jax.ShapeDtypeStruct((rows, heads * VDIM), jnp.bfloat16),
        in_specs=[smem_spec, smem_spec] + [any_spec] * 5 + [vmem_spec] * 2,
        out_specs=vmem_spec,
        scratch_shapes=[
            land,
            land,
            pltpu.VMEM((head_count,) + low.shape, jnp.bfloat16),
            pltpu.VMEM((rows, depth), jnp.bfloat16),
            pltpu.VMEM((2, depth, 2 * (NOPE + ROPE)), jnp.bfloat16),
            pltpu.VMEM(key_absorb.shape, jnp.bfloat16),
            pltpu.VMEM(value_absorb.shape, jnp.bfloat16),
            pltpu.VMEM((heads, rows, padded), jnp.bfloat16),
            pltpu.VMEM((padded, count), jnp.bfloat16),
            pltpu.VMEM((count, LATENT), jnp.bfloat16),
            pltpu.VMEM((blocks, heads, QBLK, VDIM), jnp.float32),
            pltpu.VMEM((blocks, heads, QBLK, 1), jnp.float32),
            pltpu.VMEM((blocks, heads, QBLK, 1), jnp.float32),
            dma((2, subs, n)),
            dma((2, subs, n)),
            dma((2, subs, n, lanes_x)),
            dma((2, subs, n, lanes_x)),
            dma((2, subs, n, lanes_x)),
            dma((2, subs, n, lanes_x)),
            dma((2, lanes_x)),
            dma((2, lanes_x)),
            dma((2,)),
            dma((2,)),
        ],
        compiler_params=pltpu.CompilerParams(
            collective_id=1, has_side_effects=True, vmem_limit_bytes=62 * 1024 * 1024
        ),
        cost_estimate=pl.CostEstimate(
            flops=2 * rows * heads * TOPT * TILE * (padded + LATENT),
            bytes_accessed=2 * (q_up.size + 2 * key_absorb.size),
            transcendentals=rows * heads * TOPT * TILE,
        ),
        name="exchange_attend",
    )(early, late, found, low, q_up, key_absorb, value_absorb, cosine, sine)


def slot_plan(picks, tiles_dev, seq_count, cap):
    total = picks.shape[0]
    half = cap // 2
    order = jnp.arange(total, dtype=jnp.int32)
    block = order // TOPT
    owner = picks // tiles_dev
    same = picks[:, None] == picks[None, :]
    first = jnp.min(jnp.where(same, order[None, :], total), axis=1)
    fresh = first == order
    shared = jnp.sum(same.astype(jnp.int32), axis=1) > 1
    kind = jnp.where(shared, 2, block)
    owned = owner[:, None] == jnp.arange(seq_count, dtype=jnp.int32)[None, :]

    def tally(which):
        hit = owned & (fresh & (kind == which))[:, None]
        return jnp.sum(hit.astype(jnp.int32), axis=0)

    tallies = [tally(which) for which in range(3)]
    odd_a, odd_b, odd_c = [size % 2 for size in tallies]
    split = odd_a * odd_b * (1 - odd_c)
    seqs = jnp.arange(seq_count, dtype=jnp.int32)
    turn = jnp.sum(jnp.where(seqs[None, :] < seqs[:, None], split[None, :], 0), axis=1) % 2
    up_a = jnp.where(odd_c == 1, odd_b, jnp.where(odd_b == 1, turn, 1))
    up_b = jnp.where(odd_c == 1, 0, jnp.where(odd_a == 1, 1 - turn, 1))
    early_a = tallies[0] // 2 + odd_a * up_a
    early_b = tallies[1] // 2 + odd_b * up_b
    early_c = (tallies[2] + 1) // 2
    rest_a, rest_b = tallies[0] - early_a, tallies[1] - early_b
    zero = jnp.zeros_like(early_a)
    quotas = jnp.stack([early_a, early_b, early_c])
    starts = jnp.stack([zero, early_a, early_a + early_b])
    rests = jnp.stack([zero, rest_a, rest_a + rest_b])
    chosen = owned[:, None, :] & (kind[:, None] == jnp.arange(3)[None, :])[:, :, None]

    def look(table):
        return jnp.sum(jnp.where(chosen, table[None], 0), axis=(1, 2))

    quota, start, rest = look(quotas), look(starts), look(rests)
    before = (
        (owner[:, None] == owner[None, :])
        & (kind[:, None] == kind[None, :])
        & fresh[None, :]
        & (order[None, :] < first[:, None])
    )
    index = jnp.sum(before.astype(jnp.int32), axis=1)
    early = index < quota
    spot = jnp.where(early, start + index, rest + index - quota)
    slot = owner * cap + jnp.where(early, spot, half + spot)
    hit = (slot[:, None] == jnp.arange(seq_count * cap, dtype=jnp.int32)[None, :]) & fresh[:, None]
    ask = jnp.sum(jnp.where(hit, (picks % tiles_dev)[:, None], 0), axis=0)
    land = owner * half + spot
    earlier = (block[:, None] == block[None, :]) & (order[None, :] < order[:, None])
    seen = jnp.sum((earlier & early[None, :]).astype(jnp.int32), axis=1)
    now = early & (seen < TOPT // 2)
    position = jnp.sum((earlier & (now[None, :] == now[:, None])).astype(jnp.int32), axis=1)
    position = block * (TOPT // 2) + position
    places = jnp.arange(total // 2, dtype=jnp.int32)
    at = position[:, None] == places[None, :]
    first_table = jnp.sum(jnp.where(at & now[:, None], land[:, None], 0), axis=0)
    later = at & ~now[:, None]
    fields = jnp.stack(
        [jnp.where(early, land, 0), jnp.where(early, 0, land), early.astype(jnp.int32)], axis=1
    )
    second_table = jnp.sum(jnp.where(later[:, :, None], fields[:, None, :], 0), axis=0)
    return ask.reshape(seq_count, cap), first_table, second_table.reshape(-1)


def body(q_low, q_gain, q_up, key_absorb, value_absorb, latent_cache, tile_picks):
    rows = q_low.shape[0]
    width = latent_cache.shape[1]
    seq_count = lax.axis_size("seq")
    tiles_dev = latent_cache.shape[0] // TILE
    picks = tile_picks.reshape(-1)
    count = picks.shape[0]
    cap = max(2, 2 * count // seq_count)
    ask, early, late = slot_plan(picks, tiles_dev, seq_count, cap)
    ask = jnp.pad(ask, ((0, 0), (0, LANES - cap))).reshape(seq_count, 1, LANES)
    serve = exchange_requests(ask).reshape(seq_count, LANES)[:, :cap]
    share = width // lax.axis_size("head")
    columns = lax.dynamic_slice_in_dim(latent_cache, lax.axis_index("head") * share, share, 1)
    cache_tiles = columns.T.reshape(share, tiles_dev, TILE).transpose(1, 0, 2)
    found = jnp.take(cache_tiles, serve, axis=0, mode="clip")
    low = jnp.concatenate(
        [q_low, jnp.broadcast_to(q_gain[None, :], (SUBLANES, q_gain.shape[0]))], axis=0
    )
    context = latent_cache.shape[0] * seq_count
    positions = context + lax.axis_index("seq") * rows + jnp.arange(rows, dtype=jnp.int32)
    cosine, sine = rotary_tables(positions)
    return exchange_and_attend(
        early, late, found, low, q_up, key_absorb, value_absorb, cosine, sine
    )


def solution(mesh):
    in_specs = (
        P("seq", "head"),
        P("head"),
        P(None, "head"),
        P("head", None, None),
        P("head", None, None),
        P("seq", None),
        P("seq", None),
    )
    out_specs = P("seq", "head")
    return jax.shard_map(body, mesh=mesh, in_specs=in_specs, out_specs=out_specs, check_vma=False)
```
